32 devices in a mesh: dp: 8 (over y, x, core), tensor: 4 (over z).
Axes of the slice: x: 2, y: 2, z: 4, core: 2. Of those that a mesh axis runs over, the one named last changes fastest.
Arguments:
- proxy_hidden: bfloat16 [384, 4096], P('dp', 'tensor'), may hold values from -176.625 to 176.625
- reference_hidden: bfloat16 [384, 4096], P('dp', 'tensor'), may hold values from -176.625 to 176.625
- proxy_head: bfloat16 [16032, 4096], P(('dp', 'tensor')), may hold values from -0.09375 to 0.09375
- reference_head: bfloat16 [16032, 4096], P(('dp', 'tensor')), may hold values from -0.09375 to 0.09375
- targets: int32 [384], P('dp'), may hold values from 0 to 16031
- domains: int32 [384], P('dp'), may hold values from 0 to 127
- keep_mask: int32 [384], P('dp'), may hold values 0 or 1
- prior_weights: float32 [128], replicated, may hold values from 0.5 to 2
Outputs:
- excess: float32 [384], P('dp')
- log_weights: float32 [128], replicated
The draws below stay inside these ranges and needn't reach their ends.
All inputs are finite; a program needn't handle non-finite values. No bound on the sum of `keep_mask` on one device may be relied on, other than what follows from the above.
Results may differ from the reference program's by a relative error of at most 0.00045.
Values may be sent and summed in bfloat16 or wider, within the bound.
A program may use at most 128 MiB of HBM per device.

```python
import math
import jax
import jax.numpy as jnp
from jax import lax

D = 4096
VOCAB_DEV = 501
DOMAINS = 128
STEPS = 3
TOKENS = 384
VOCAB = 16032


def head_rows(key, salt, rows):
    base = jax.random.fold_in(key, salt)

    def one_row(row_id):
        values = jax.random.normal(jax.random.fold_in(base, row_id), (D,), jnp.float32)
        return jnp.clip(values, -6.0, 6.0) * D ** (-0.5)
    return jax.vmap(one_row)(rows)


def hidden_matrix(key, salt):
    base = jax.random.fold_in(key, salt)
    values = jnp.clip(jax.random.normal(base, (TOKENS, D), jnp.float32), -6.0, 6.0) * 3.0
    return values.astype(jnp.bfloat16)


def draw_proxy_head(key, part):
    return head_rows(key, 101, jnp.arange(VOCAB, dtype=jnp.int32)).astype(jnp.bfloat16)


def draw_reference_head(key, part):
    return head_rows(key, 102, jnp.arange(VOCAB, dtype=jnp.int32)).astype(jnp.bfloat16)


def draw_proxy_hidden(key, part):
    return hidden_matrix(key, 201)


def draw_reference_hidden(key, part):
    return hidden_matrix(key, 202)


def set_ends(entries, key, smallest, largest):
    longest = entries.shape.index(max(entries.shape))
    spots = []
    for shift in (0, 1):
        where = [jax.random.randint(jax.random.fold_in(key, axis), (), 0, length) for axis, length in enumerate(entries.shape)]
        where[longest] = (where[longest] + shift) % entries.shape[longest]
        spots.append(tuple(where))
    return entries.at[spots[0]].set(smallest).at[spots[1]].set(largest)


def setup_inputs(seed: int = 0) -> dict:
    streams_of = jax.random.split(jax.random.key(seed), 9)
    return {
        "proxy_hidden": draw_proxy_hidden(jax.random.fold_in(streams_of[8], 71), 0),
        "reference_hidden": draw_reference_hidden(jax.random.fold_in(streams_of[8], 71), 0),
        "proxy_head": draw_proxy_head(jax.random.fold_in(streams_of[8], 71), 0),
        "reference_head": draw_reference_head(jax.random.fold_in(streams_of[8], 71), 0),
        "targets": set_ends(jax.random.randint(streams_of[4], (TOKENS,), 0, VOCAB), jax.random.fold_in(streams_of[4], 1), 0, VOCAB - 1).astype(jnp.int32),
        "domains": set_ends(jax.random.randint(streams_of[5], (TOKENS,), 0, DOMAINS), jax.random.fold_in(streams_of[5], 1), 0, DOMAINS - 1).astype(jnp.int32),
        "keep_mask": set_ends((jax.random.randint(streams_of[6], (TOKENS,), 0, 8) < 7).astype(jnp.int32), jax.random.fold_in(streams_of[6], 1), 0, 1),
        "prior_weights": jnp.clip(jnp.exp(jax.random.uniform(streams_of[7], (DOMAINS,), jnp.float32, math.log(0.5), math.log(2.0))), 0.5, 2.0),
    }


step_size = 1.0
smoothing = 0.001


def model_loss(hidden, head, targets):
    blocks = VOCAB // VOCAB_DEV
    grouped = head.reshape(blocks, VOCAB_DEV, D)
    firsts = jnp.arange(blocks, dtype=jnp.int32) * VOCAB_DEV
    columns = jnp.arange(VOCAB_DEV, dtype=jnp.int32)

    def visit(state, inputs):
        run_peak, run_total, run_hit = state
        block_head, first_col = inputs
        logits = lax.dot_general(hidden, block_head, (((1,), (1,)), ((), ())), preferred_element_type=jnp.float32)
        new_peak = jnp.maximum(run_peak, jnp.max(logits, axis=1))
        run_total = run_total * jnp.exp(run_peak - new_peak) + jnp.sum(jnp.exp(logits - new_peak[:, None]), axis=1)
        matched = (targets - first_col)[:, None] == columns[None, :]
        run_hit = run_hit + jnp.sum(jnp.where(matched, logits, 0.0), axis=1)
        return (new_peak, run_total, run_hit), None

    zeros_row = jnp.zeros((TOKENS,), jnp.float32)
    start_state = (jnp.full((TOKENS,), -jnp.inf, jnp.float32), zeros_row, zeros_row)
    final_state, _unused = lax.scan(visit, start_state, (grouped, firsts))
    final_peak, final_total, final_hit = final_state
    return final_peak + jnp.log(final_total) - final_hit


def update_weights(prior_weights, clipped, domains, keep):
    weights = prior_weights / jnp.sum(prior_weights)
    batch_rows = clipped.shape[0] // STEPS
    labels = jnp.arange(DOMAINS, dtype=jnp.int32)
    for section_index in range(STEPS):
        row_start = section_index * batch_rows
        block_loss = clipped[row_start:row_start + batch_rows]
        block_keep = keep[row_start:row_start + batch_rows]
        member = (domains[row_start:row_start + batch_rows][:, None] == labels[None, :]).astype(jnp.float32)
        domain_sum = jnp.dot(block_loss, member, precision=lax.Precision.HIGHEST)
        domain_count = jnp.dot(block_keep, member, precision=lax.Precision.HIGHEST)
        domain_gain = domain_sum / jnp.maximum(domain_count, 1.0)
        raised = weights * jnp.exp(step_size * domain_gain)
        weights = (1.0 - smoothing) * raised / jnp.sum(raised) + smoothing / DOMAINS
    return jnp.log(weights)


def reference(proxy_hidden, reference_hidden, proxy_head, reference_head, targets, domains, keep_mask, prior_weights):
    proxy_loss = model_loss(proxy_hidden, proxy_head, targets)
    reference_loss = model_loss(reference_hidden, reference_head, targets)
    keep = keep_mask.astype(jnp.float32)
    loss_gap = proxy_loss - reference_loss
    excess = loss_gap * keep
    clipped = jnp.maximum(loss_gap, 0.0) * keep
    log_weights = update_weights(prior_weights, clipped, domains, keep)
    return excess, log_weights
```

```python
import functools

import jax
import jax.numpy as jnp
from jax import lax
from jax.experimental import pallas as pl
from jax.experimental.pallas import tpu as pltpu
from jax.sharding import PartitionSpec as P

STEPS = 3
MESH = pl.DeviceIdType.MESH
step_size = 1.0
smoothing = 0.001
LAG = 6


def arrival(position, size, index):
    if index == 0:
        return 0
    near = jnp.minimum(position, size - 1 - position)
    far_sign = jnp.where(2 * position < size - 1, 1, -1)
    half = (index + 1) // 2
    paired = -half if index % 2 else half
    return jnp.where(index <= 2 * near, paired, far_sign * (index - near))


def kernel(
    sizes,
    hidden0, hidden1, head0, head1, targets, domains, keep, prior,
    excess_out, weights_out,
    gath, heads, acc, meta_src, meta, stats,
    load_sem, head_sem, item_send, item_recv, meta_send, meta_recv, stat_send, stat_recv,
):
    rows_a, rows_b, nz, tok = sizes
    ncol = rows_a * rows_b
    ndp = 2 * ncol
    ndev = ndp * nz
    voc = head0.shape[0]
    feats = hidden0.shape[1]
    pair = 2 * tok
    dom = prior.shape[1]
    dp = lax.axis_index("dp")
    z = lax.axis_index("tensor")
    core = dp % 2
    col = dp // 2
    a, b = col // rows_b, col % rows_b
    me = dp * nz + z

    def own_rows(c):
        return pl.ds(pl.multiple_of(c * tok, tok), tok)

    loads = []
    for m, ref in enumerate((hidden0, hidden1)):
        loads.append(pltpu.make_async_copy(ref, gath.at[m, col, z, own_rows(core)], load_sem.at[m]))
        loads[-1].start()
    head_loads = []
    for k in range(nz):
        for m, ref in enumerate((head0, head1)):
            head_loads.append(
                pltpu.make_async_copy(ref.at[:, pl.ds(k * feats, feats)], heads.at[m, k], head_sem.at[m, k])
            )
            head_loads[-1].start()

    lane = lax.broadcasted_iota(jnp.int32, (1, 128), 1)
    meta_src[...] = jnp.zeros_like(meta_src)
    for r, ref in enumerate((targets, domains, keep)):
        meta_src[:, r * 128 : r * 128 + tok] = ref[...]
    barrier = pltpu.get_barrier_semaphore()

    met_count = [jnp.int32(1)]

    def greet(target, ok):
        if ok is not True:
            met_count[0] = met_count[0] + jnp.where(ok, 1, 0)

            @pl.when(ok)
            def _():
                pl.semaphore_signal(barrier, inc=1, device_id=target, device_id_type=MESH)

            return
        met_count[0] = met_count[0] + 1
        pl.semaphore_signal(barrier, inc=1, device_id=target, device_id_type=MESH)

    pl.semaphore_signal(
        barrier, inc=1, device_id=((a * rows_b + b) * 2 + 1 - core, z), device_id_type=MESH
    )
    for axis, size, at in (("a", rows_a, a), ("b", rows_b, b), ("z", nz, z)):
        moves = [] if size == 1 else [(1 - at, True)]
        if size > 2:
            moves = [(at + 1, at < size - 1), (at - 1, at > 0)]
        for to, ok in moves:
            spot = {"a": a, "b": b, "z": z}
            spot[axis] = to
            greet(((spot["a"] * rows_b + spot["b"]) * 2 + core, spot["z"]), ok)
    pl.semaphore_wait(barrier, met_count[0])
    for copy in loads:
        copy.wait()

    sent = [jnp.int32(0)]

    def item_copy(m, colp, zp, c, target):
        slot = gath.at[m, colp, zp, own_rows(c)]
        return pltpu.make_async_remote_copy(
            src_ref=slot, dst_ref=slot, send_sem=item_send, recv_sem=item_recv.at[m, colp, zp, c],
            device_id=target, device_id_type=MESH,
        )

    def place(aa, bb, cc, zz):
        return ((aa * rows_b + bb) * 2 + cc, zz)

    here = {"a": a, "b": b, "z": z}
    length = {"a": rows_a, "b": rows_b, "z": nz}

    def send(m, colp, zp, axis, where_to, ok):
        spot = dict(here)
        spot[axis] = where_to
        target = place(spot["a"], spot["b"], core, spot["z"])
        if ok is True:
            sent[0] = sent[0] + 1
            item_copy(m, colp, zp, core, target).start()
            return
        sent[0] = sent[0] + jnp.where(ok, 1, 0)

        @pl.when(ok)
        def _():
            item_copy(m, colp, zp, core, target).start()

    def spread(m, colp, zp, axis):
        size, at = length[axis], here[axis]
        if size == 2:
            send(m, colp, zp, axis, 1 - at, True)
        elif size > 2:
            send(m, colp, zp, axis, at + 1, at < size - 1)
            send(m, colp, zp, axis, at - 1, at > 0)

    def onward(m, colp, zp, axis, off):
        size, at = length[axis], here[axis]
        if size > 2:
            ok = jnp.where(off < 0, at < size - 1, at > 0)
            send(m, colp, zp, axis, jnp.where(off < 0, at + 1, at - 1), ok)

    events = []
    for m in (0, 1):
        first, second = ("b", "a") if m == 0 else ("a", "b")
        for iz in range(nz):
            for i1 in range(length[first]):
                for i2 in range(length[second]):
                    key = (4.2 if i1 + i2 == 0 else 6.3) * iz
                    key += 3.8 * i1 + 6.0 * i2 + 0.2 * i1 * i2
                    events.append((key, m, iz, i1, i2))
    events.sort()

    def locate(event):
        _, m, iz, i1, i2 = event
        first, second = ("b", "a") if m == 0 else ("a", "b")
        off_z = arrival(z, nz, iz)
        off1 = arrival(here[first], length[first], i1)
        off2 = arrival(here[second], length[second], i2)
        spot = {first: here[first] + off1, second: here[second] + off2}
        return m, spot["a"] * rows_b + spot["b"], z + off_z, first, second, off_z, off1, off2

    def take(event):
        _, _, iz, i1, i2 = event
        m, colp, zp, first, second, off_z, off1, off2 = locate(event)
        partner = place(a, b, 1 - core, z)
        if iz + i1 + i2:
            item_copy(m, colp, zp, core, partner).wait_recv()
        if i2:
            onward(m, colp, zp, second, off2)
        elif i1:
            onward(m, colp, zp, first, off1)
            spread(m, colp, zp, second)
        else:
            if iz:
                onward(m, colp, zp, "z", off_z)
            else:
                spread(m, colp, zp, "z")
            spread(m, colp, zp, first)
            spread(m, colp, zp, second)
        sent[0] = sent[0] + 1
        item_copy(m, colp, zp, core, partner).start()

    def multiply(m, colp, zp, fresh):
        part = lax.dot_general(
            heads[m, zp], gath[m, colp, zp], (((1,), (1,)), ((), ())),
            preferred_element_type=jnp.float32,
        )
        if fresh:
            acc[m, colp] = part
        else:
            acc[m, colp] += part

    def meta_copy(k):
        other = lax.rem(dp + k, ndp)
        return pltpu.make_async_remote_copy(
            src_ref=meta_src, dst_ref=meta.at[dp], send_sem=meta_send, recv_sem=meta_recv,
            device_id=(other, z), device_id_type=MESH,
        )

    def stat_copy(colp, k):
        other = lax.rem(me + k, ndev)
        return pltpu.make_async_remote_copy(
            src_ref=stats.at[ndev - 1, colp], dst_ref=stats.at[k - 1, colp],
            send_sem=stat_send, recv_sem=stat_recv,
            device_id=(other // nz, other % nz), device_id_type=MESH,
        )

    def meta_row(colp, r):
        low = meta[2 * colp, :, r * 128 : (r + 1) * 128]
        high = meta[2 * colp + 1, :, r * 128 : (r + 1) * 128]
        return low + pltpu.roll(high, tok, 1)

    base = me * voc
    entries = lax.broadcasted_iota(jnp.int32, (voc, pair), 0)

    def finish(colp):
        local_target = (meta_row(colp, 0) - base)[:, :pair]
        matched = entries == local_target
        lse, hit = [], []
        for m in (0, 1):
            logits = acc[m, colp]
            peak = jnp.max(logits, axis=0, keepdims=True)
            lse.append(peak + jnp.log(jnp.sum(jnp.exp(logits - peak), axis=0, keepdims=True)))
            hit.append(jnp.sum(jnp.where(matched, logits, 0.0), axis=0, keepdims=True))
        for r, row in enumerate((lse[0], lse[1], hit[0] - hit[1])):
            stats[ndev - 1, colp, :, r * 128 : r * 128 + pair] = row

    def tell_all(colp):
        def tell(k, carry):
            stat_copy(colp, k).start()
            return carry

        lax.fori_loop(1, ndev, tell, 0)

    waiting = []
    seen_head = set()
    done = {}
    met = [False]
    meta_sent = [False]
    heard = set()
    untold = []

    def work(event):
        m, colp, zp = locate(event)[:3]
        _, _, iz, i1, i2 = event
        item_copy(m, colp, zp, 1 - core, place(a, b, 1 - core, z)).wait_recv()
        if (m, iz) not in seen_head:
            seen_head.add((m, iz))
            pltpu.make_async_copy(
                (head0, head1)[m].at[:, pl.ds(pl.multiple_of(zp * feats, 128), feats)],
                heads.at[m, zp], head_sem.at[m, zp],
            ).wait()
        return m, colp, zp

    small = ncol * nz <= 32
    offs = {}
    for number, event in enumerate(events):
        take(event)
        if number == 1:
            meta[dp] = meta_src[...]
        waiting.append(event)
        while len(waiting) > LAG or (waiting and number == len(events) - 1):
            past = waiting.pop(0)
            m, colp, zp = work(past)
            ia, ib = (past[4], past[3]) if m == 0 else (past[3], past[4])
            count = done.get((m, ia, ib), 0)
            done[m, ia, ib] = count + 1
            heard.add((past[2], ia, ib))
            if not meta_sent[0] and len([k for k in heard if k[0] == 0]) == ncol:
                meta_sent[0] = True
                for k in range(1, ndp):
                    meta_copy(k).start()
            if not small:
                continue
            multiply(m, colp, zp, count == 0)
            if done.get((0, ia, ib), 0) == nz and done.get((1, ia, ib), 0) == nz:
                if not met[0]:
                    met[0] = True
                    pltpu.make_async_copy(
                        meta.at[pl.ds(0, ndp - 1)], meta.at[pl.ds(0, ndp - 1)], meta_recv
                    ).wait()
                finish(colp)
                untold.append(colp)
            if len(heard) == ncol * nz:
                while untold:
                    tell_all(untold.pop(0))
    if not small:
        pltpu.make_async_copy(meta.at[pl.ds(0, ndp - 1)], meta.at[pl.ds(0, ndp - 1)], meta_recv).wait()

        def whole_column(colp, carry):
            for m in (0, 1):
                acc[m, colp] = jnp.zeros((voc, pair), jnp.float32)

                def chunk(zp, inner):
                    multiply(m, colp, zp, False)
                    return inner

                lax.fori_loop(0, nz, chunk, 0)
            finish(colp)
            tell_all(colp)
            return carry

        lax.fori_loop(0, ncol, whole_column, 0)

    labels = lax.broadcasted_iota(jnp.int32, (dom, 128), 0)
    row_id = lax.broadcasted_iota(jnp.int32, (8, 128), 0)
    batch = ncol * pair // STEPS
    valid = lane < pair

    remote = stats.at[pl.ds(0, ndev - 1)]
    pltpu.make_async_copy(remote, remote, stat_recv).wait()

    total = jnp.zeros((8, dom), jnp.float32)
    for k in range(ncol):
        row = [stats[:, k, :, r * 128 : (r + 1) * 128] for r in range(3)]
        lse = []
        for m in (0, 1):
            peak = jnp.max(row[m], axis=0)
            lse.append(peak + jnp.log(jnp.sum(jnp.exp(row[m] - peak[None]), axis=0)))
        kept = meta_row(k, 2).astype(jnp.float32)
        gap = jnp.where(valid, lse[0] - lse[1] - jnp.sum(row[2], axis=0), 0.0)
        excess = gap * kept
        clipped = jnp.maximum(gap, 0.0) * kept

        @pl.when(k == col)
        def _():
            mine = jnp.where(core == 0, excess, pltpu.roll(excess, 128 - tok, 1))
            excess_out[...] = mine[:, :tok]

        step_of = (lane + k * pair) // batch
        member = ((meta_row(k, 1) == labels) & valid).astype(jnp.float32)
        values = jnp.where(row_id < STEPS, clipped, kept)
        values = jnp.where((row_id % STEPS == step_of) & (row_id < 2 * STEPS) & valid, values, 0.0)
        total = total + lax.dot_general(
            values, member, (((1,), (1,)), ((), ())),
            precision=lax.Precision.HIGHEST, preferred_element_type=jnp.float32,
        )
    weights = prior[...] / jnp.sum(prior[...], axis=1, keepdims=True)
    for s in range(STEPS):
        gain = total[s : s + 1] / jnp.maximum(total[STEPS + s : STEPS + s + 1], 1.0)
        raised = weights * jnp.exp(step_size * gain)
        weights = (1.0 - smoothing) * raised / jnp.sum(raised, axis=1, keepdims=True) + smoothing / dom
    weights_out[...] = jnp.log(weights)

    def drain_items(k, carry):
        item_copy(0, 0, 0, 0, place(a, b, 1 - core, z)).wait_send()
        return carry

    lax.fori_loop(0, sent[0], drain_items, 0)
    pltpu.make_async_copy(meta.at[pl.ds(0, ndp - 1)], meta.at[pl.ds(0, ndp - 1)], meta_send).wait()
    pltpu.make_async_copy(remote, remote, stat_send).wait()


def local(sizes, h0, h1, w0, w1, targets, domains, keep, prior):
    rows_a, rows_b, nz, tok = sizes
    ncol = rows_a * rows_b
    ndp = 2 * ncol
    ndev = ndp * nz
    voc = w0.shape[0]
    feats = h0.shape[1]
    anywhere = pl.BlockSpec(memory_space=pl.ANY)
    vmem = pl.BlockSpec(memory_space=pltpu.VMEM)
    excess, weights = pl.pallas_call(
        functools.partial(kernel, sizes),
        out_shape=(
            jax.ShapeDtypeStruct((1, tok), jnp.float32),
            jax.ShapeDtypeStruct((1, prior.shape[0]), jnp.float32),
        ),
        in_specs=[anywhere] * 4 + [vmem] * 4,
        out_specs=(vmem, vmem),
        scratch_shapes=[
            pltpu.VMEM((2, ncol, nz, 2 * tok, feats), jnp.bfloat16),
            pltpu.VMEM((2, nz, voc, feats), jnp.bfloat16),
            pltpu.VMEM((2, ncol, voc, 2 * tok), jnp.float32),
            pltpu.VMEM((1, 384), jnp.int32),
            pltpu.VMEM((ndp, 1, 384), jnp.int32),
            pltpu.VMEM((ndev, ncol, 1, 384), jnp.float32),
            pltpu.SemaphoreType.DMA((2,)),
            pltpu.SemaphoreType.DMA((2, nz)),
            pltpu.SemaphoreType.DMA,
            pltpu.SemaphoreType.DMA((2, ncol, nz, 2)),
            pltpu.SemaphoreType.DMA,
            pltpu.SemaphoreType.DMA,
            pltpu.SemaphoreType.DMA,
            pltpu.SemaphoreType.DMA,
        ],
        compiler_params=pltpu.CompilerParams(
            collective_id=0, has_side_effects=True, vmem_limit_bytes=66_000_000
        ),
    )(h0, h1, w0, w1, targets[None], domains[None], keep[None], prior[None])
    return excess[0], weights[0]


def solution(mesh):
    ndp, nz = mesh.shape["dp"], mesh.shape["tensor"]
    ncol = ndp // 2
    rows_b = max(k for k in range(1, ncol + 1) if ncol % k == 0 and k * k <= ncol)

    def body(h0, *rest):
        return local((ncol // rows_b, rows_b, nz, h0.shape[0]), h0, *rest)

    in_specs = (
        P("dp", "tensor"),
        P("dp", "tensor"),
        P(("dp", "tensor"), None),
        P(("dp", "tensor"), None),
        P("dp"),
        P("dp"),
        P("dp"),
        P(),
    )
    return jax.shard_map(body, mesh=mesh, in_specs=in_specs, out_specs=(P("dp"), P()), check_vma=False)
```

```python
import functools

import jax
import jax.numpy as jnp
from jax import lax
from jax.experimental import pallas as pl
from jax.experimental.pallas import tpu as pltpu
from jax.sharding import PartitionSpec as P

STEPS = 3
MESH = pl.DeviceIdType.MESH
step_size = 1.0
smoothing = 0.001
LAG = 6
ROUTES = ("Za", "Qb", "Zb", "Qa")
PLAN_LAG = 8
PLAN = (
    (2, 0, 0, 0, 0), (3, 0, 0, 0, 0), (0, 0, 0, 0, 0), (1, 0, 0, 0, 0), (2, 0, 0, 1, 1),
    (3, 1, 0, 0, 0), (3, 0, 1, 0, 0), (2, 0, 1, 0, 0), (0, 0, 1, 0, 0), (0, 0, 0, 1, 1),
    (3, 0, 0, 1, 1), (2, 0, 0, 2, -1), (1, 0, 1, 0, 0), (2, 1, 0, 0, 0), (1, 1, 0, 0, 0),
    (0, 1, 0, 0, 0), (2, 0, 1, 1, 1), (3, 0, 0, 2, -1), (1, 0, 0, 1, 1), (0, 0, 0, 2, -1),
    (2, 1, 0, 1, 1), (3, 1, 1, 0, 0), (0, 0, 1, 1, 1), (2, 1, 1, 0, 0), (0, 1, 0, 1, 1),
    (1, 0, 0, 2, -1), (2, 0, 0, 3, 2), (2, 1, 0, 2, -1), (1, 0, 1, 1, -1), (3, 1, 0, 1, -1),
    (3, 1, 0, 2, 1), (2, 0, 1, 2, -1), (1, 1, 1, 0, 0), (0, 0, 0, 3, 2), (3, 0, 1, 1, 1),
    (2, 1, 1, 1, 1), (0, 1, 1, 0, 0), (3, 0, 0, 3, 2), (1, 1, 0, 1, 1), (3, 0, 1, 2, -1),
    (1, 0, 0, 3, 2), (0, 0, 1, 2, -1), (0, 1, 0, 2, -1), (1, 1, 0, 2, -1), (1, 0, 1, 2, 1),
    (0, 1, 1, 1, 1), (3, 1, 0, 3, 2), (2, 0, 1, 3, 2), (2, 1, 0, 3, 2), (3, 1, 1, 1, -1),
    (1, 1, 1, 1, -1), (1, 0, 1, 3, 2), (0, 1, 0, 3, 2), (1, 1, 0, 3, 2), (2, 1, 1, 2, -1),
    (0, 0, 1, 3, 2), (0, 1, 1, 2, -1), (3, 1, 1, 2, 1), (3, 0, 1, 3, 2), (2, 1, 1, 3, 2),
    (3, 1, 1, 3, 2), (1, 1, 1, 2, 1), (0, 1, 1, 3, 2), (1, 1, 1, 3, 2),
)


def arrival(position, size, index):
    if index == 0:
        return 0
    near = jnp.minimum(position, size - 1 - position)
    far_sign = jnp.where(2 * position < size - 1, 1, -1)
    half = (index + 1) // 2
    paired = -half if index % 2 else half
    return jnp.where(index <= 2 * near, paired, far_sign * (index - near))


def kernel(
    sizes,
    hidden0, hidden1, head0, head1, targets, domains, keep, prior,
    excess_out, weights_out,
    gath, heads, acc, meta_src, meta, stats,
    load_sem, head_sem, item_send, item_recv, meta_send, meta_recv, stat_send, stat_recv,
):
    rows_a, rows_b, nz, tok = sizes
    ncol = rows_a * rows_b
    ndp = 2 * ncol
    ndev = ndp * nz
    voc = head0.shape[0]
    feats = hidden0.shape[1]
    pair = 2 * tok
    dom = prior.shape[1]
    dp = lax.axis_index("dp")
    z = lax.axis_index("tensor")
    core = dp % 2
    col = dp // 2
    a, b = col // rows_b, col % rows_b
    me = dp * nz + z

    def own_rows(c):
        return pl.ds(pl.multiple_of(c * tok, tok), tok)

    loads = []
    for m, ref in enumerate((hidden0, hidden1)):
        loads.append(pltpu.make_async_copy(ref, gath.at[m, col, z, own_rows(core)], load_sem.at[m]))
        loads[-1].start()
    head_loads = []
    for k in range(nz):
        for m, ref in enumerate((head0, head1)):
            head_loads.append(
                pltpu.make_async_copy(ref.at[:, pl.ds(k * feats, feats)], heads.at[m, k], head_sem.at[m, k])
            )
            head_loads[-1].start()

    lane = lax.broadcasted_iota(jnp.int32, (1, 128), 1)
    meta_src[...] = jnp.zeros_like(meta_src)
    for r, ref in enumerate((targets, domains, keep)):
        meta_src[:, r * 128 : r * 128 + tok] = ref[...]
    barrier = pltpu.get_barrier_semaphore()

    def greet(k, carry):
        other = lax.rem(me + k, ndev)
        pl.semaphore_signal(barrier, inc=1, device_id=(other // nz, other % nz), device_id_type=MESH)
        return carry

    lax.fori_loop(1, ndev, greet, 0)
    pl.semaphore_wait(barrier, ndev - 1)
    for copy in loads:
        copy.wait()

    sent = [jnp.int32(0)]

    def item_copy(m, colp, zp, c, target):
        slot = gath.at[m, colp, zp, own_rows(c)]
        return pltpu.make_async_remote_copy(
            src_ref=slot, dst_ref=slot, send_sem=item_send, recv_sem=item_recv.at[m, colp, zp, c],
            device_id=target, device_id_type=MESH,
        )

    def place(aa, bb, cc, zz):
        return ((aa * rows_b + bb) * 2 + cc, zz)

    here = {"a": a, "b": b, "z": z}
    length = {"a": rows_a, "b": rows_b, "z": nz}

    def send(m, colp, zp, axis, where_to, ok):
        spot = dict(here)
        spot[axis] = where_to
        target = place(spot["a"], spot["b"], core, spot["z"])
        if ok is True:
            sent[0] = sent[0] + 1
            item_copy(m, colp, zp, core, target).start()
            return
        sent[0] = sent[0] + jnp.where(ok, 1, 0)

        @pl.when(ok)
        def _():
            item_copy(m, colp, zp, core, target).start()

    def spread(m, colp, zp, axis):
        size, at = length[axis], here[axis]
        if size == 2:
            send(m, colp, zp, axis, 1 - at, True)
        elif size > 2:
            send(m, colp, zp, axis, at + 1, at < size - 1)
            send(m, colp, zp, axis, at - 1, at > 0)

    def onward(m, colp, zp, axis, off):
        size, at = length[axis], here[axis]
        if size > 2:
            ok = jnp.where(off < 0, at < size - 1, at > 0)
            send(m, colp, zp, axis, jnp.where(off < 0, at + 1, at - 1), ok)

    events = []
    for m in (0, 1):
        first, second = ("b", "a") if m == 0 else ("a", "b")
        for iz in range(nz):
            for i1 in range(length[first]):
                for i2 in range(length[second]):
                    key = (4.2 if i1 + i2 == 0 else 6.3) * iz
                    key += 3.8 * i1 + 6.0 * i2 + 0.2 * i1 * i2
                    events.append((key, m, iz, i1, i2))
    events.sort()

    def locate(event):
        _, m, iz, i1, i2 = event
        first, second = ("b", "a") if m == 0 else ("a", "b")
        off_z = arrival(z, nz, iz)
        off1 = arrival(here[first], length[first], i1)
        off2 = arrival(here[second], length[second], i2)
        spot = {first: here[first] + off1, second: here[second] + off2}
        return m, spot["a"] * rows_b + spot["b"], z + off_z, first, second, off_z, off1, off2

    def take(event):
        _, _, iz, i1, i2 = event
        m, colp, zp, first, second, off_z, off1, off2 = locate(event)
        partner = place(a, b, 1 - core, z)
        if iz + i1 + i2:
            item_copy(m, colp, zp, core, partner).wait_recv()
        if i2:
            onward(m, colp, zp, second, off2)
        elif i1:
            onward(m, colp, zp, first, off1)
            spread(m, colp, zp, second)
        else:
            if iz:
                onward(m, colp, zp, "z", off_z)
            else:
                spread(m, colp, zp, "z")
            spread(m, colp, zp, first)
            spread(m, colp, zp, second)
        sent[0] = sent[0] + 1
        item_copy(m, colp, zp, core, partner).start()

    def multiply(m, colp, zp, fresh):
        part = lax.dot_general(
            heads[m, zp], gath[m, colp, zp], (((1,), (1,)), ((), ())),
            preferred_element_type=jnp.float32,
        )
        if fresh:
            acc[m, colp] = part
        else:
            acc[m, colp] += part

    def meta_copy(k):
        other = lax.rem(dp + k, ndp)
        return pltpu.make_async_remote_copy(
            src_ref=meta_src, dst_ref=meta.at[dp], send_sem=meta_send, recv_sem=meta_recv,
            device_id=(other, z), device_id_type=MESH,
        )

    def stat_copy(colp, k):
        other = lax.rem(me + k, ndev)
        return pltpu.make_async_remote_copy(
            src_ref=stats.at[ndev - 1, colp], dst_ref=stats.at[k - 1, colp],
            send_sem=stat_send, recv_sem=stat_recv,
            device_id=(other // nz, other % nz), device_id_type=MESH,
        )

    def meta_row(colp, r):
        low = meta[2 * colp, :, r * 128 : (r + 1) * 128]
        high = meta[2 * colp + 1, :, r * 128 : (r + 1) * 128]
        return low + pltpu.roll(high, tok, 1)

    base = me * voc
    entries = lax.broadcasted_iota(jnp.int32, (voc, pair), 0)

    def finish(colp):
        local_target = (meta_row(colp, 0) - base)[:, :pair]
        matched = entries == local_target
        lse, hit = [], []
        for m in (0, 1):
            logits = acc[m, colp]
            peak = jnp.max(logits, axis=0, keepdims=True)
            lse.append(peak + jnp.log(jnp.sum(jnp.exp(logits - peak), axis=0, keepdims=True)))
            hit.append(jnp.sum(jnp.where(matched, logits, 0.0), axis=0, keepdims=True))
        for r, row in enumerate((lse[0], lse[1], hit[0] - hit[1])):
            stats[ndev - 1, colp, :, r * 128 : r * 128 + pair] = row

        def tell(k, carry):
            stat_copy(colp, k).start()
            return carry

        lax.fori_loop(1, ndev, tell, 0)

    waiting = []
    seen_head = set()
    done = {}
    met = [False]

    def work(event):
        m, colp, zp = locate(event)[:3]
        _, _, iz, i1, i2 = event
        item_copy(m, colp, zp, 1 - core, place(a, b, 1 - core, z)).wait_recv()
        if (m, iz) not in seen_head:
            seen_head.add((m, iz))
            pltpu.make_async_copy(
                (head0, head1)[m].at[:, pl.ds(pl.multiple_of(zp * feats, 128), feats)],
                heads.at[m, zp], head_sem.at[m, zp],
            ).wait()
        return m, colp, zp

    small = ncol * nz <= 32
    offs = {}
    for number, event in enumerate(events):
        take(event)
        if number == 1:
            meta[dp] = meta_src[...]
            for k in range(1, ndp):
                meta_copy(k).start()
        waiting.append(event)
        while len(waiting) > LAG or (waiting and number == len(events) - 1):
            past = waiting.pop(0)
            m, colp, zp = work(past)
            ia, ib = (past[4], past[3]) if m == 0 else (past[3], past[4])
            count = done.get((m, ia, ib), 0)
            done[m, ia, ib] = count + 1
            if not small:
                continue
            multiply(m, colp, zp, count == 0)
            if done.get((0, ia, ib), 0) == nz and done.get((1, ia, ib), 0) == nz:
                if not met[0]:
                    met[0] = True
                    pltpu.make_async_copy(
                        meta.at[pl.ds(0, ndp - 1)], meta.at[pl.ds(0, ndp - 1)], meta_recv
                    ).wait()
                finish(colp)
    if not small:
        pltpu.make_async_copy(meta.at[pl.ds(0, ndp - 1)], meta.at[pl.ds(0, ndp - 1)], meta_recv).wait()

        def whole_column(colp, carry):
            for m in (0, 1):
                acc[m, colp] = jnp.zeros((voc, pair), jnp.float32)

                def chunk(zp, inner):
                    multiply(m, colp, zp, False)
                    return inner

                lax.fori_loop(0, nz, chunk, 0)
            finish(colp)
            return carry

        lax.fori_loop(0, ncol, whole_column, 0)

    labels = lax.broadcasted_iota(jnp.int32, (dom, 128), 0)
    row_id = lax.broadcasted_iota(jnp.int32, (8, 128), 0)
    batch = ncol * pair // STEPS
    valid = lane < pair

    remote = stats.at[pl.ds(0, ndev - 1)]
    pltpu.make_async_copy(remote, remote, stat_recv).wait()

    total = jnp.zeros((8, dom), jnp.float32)
    for k in range(ncol):
        row = [stats[:, k, :, r * 128 : (r + 1) * 128] for r in range(3)]
        lse = []
        for m in (0, 1):
            peak = jnp.max(row[m], axis=0)
            lse.append(peak + jnp.log(jnp.sum(jnp.exp(row[m] - peak[None]), axis=0)))
        kept = meta_row(k, 2).astype(jnp.float32)
        gap = jnp.where(valid, lse[0] - lse[1] - jnp.sum(row[2], axis=0), 0.0)
        excess = gap * kept
        clipped = jnp.maximum(gap, 0.0) * kept

        @pl.when(k == col)
        def _():
            mine = jnp.where(core == 0, excess, pltpu.roll(excess, 128 - tok, 1))
            excess_out[...] = mine[:, :tok]

        step_of = (lane + k * pair) // batch
        member = ((meta_row(k, 1) == labels) & valid).astype(jnp.float32)
        values = jnp.where(row_id < STEPS, clipped, kept)
        values = jnp.where((row_id % STEPS == step_of) & (row_id < 2 * STEPS) & valid, values, 0.0)
        total = total + lax.dot_general(
            values, member, (((1,), (1,)), ((), ())),
            precision=lax.Precision.HIGHEST, preferred_element_type=jnp.float32,
        )
    weights = prior[...] / jnp.sum(prior[...], axis=1, keepdims=True)
    for s in range(STEPS):
        gain = total[s : s + 1] / jnp.maximum(total[STEPS + s : STEPS + s + 1], 1.0)
        raised = weights * jnp.exp(step_size * gain)
        weights = (1.0 - smoothing) * raised / jnp.sum(raised, axis=1, keepdims=True) + smoothing / dom
    weights_out[...] = jnp.log(weights)

    def drain_items(k, carry):
        item_copy(0, 0, 0, 0, place(a, b, 1 - core, z)).wait_send()
        return carry

    lax.fori_loop(0, sent[0], drain_items, 0)
    pltpu.make_async_copy(meta.at[pl.ds(0, ndp - 1)], meta.at[pl.ds(0, ndp - 1)], meta_send).wait()
    pltpu.make_async_copy(remote, remote, stat_send).wait()


def local(sizes, h0, h1, w0, w1, targets, domains, keep, prior):
    rows_a, rows_b, nz, tok = sizes
    ncol = rows_a * rows_b
    ndp = 2 * ncol
    ndev = ndp * nz
    voc = w0.shape[0]
    feats = h0.shape[1]
    anywhere = pl.BlockSpec(memory_space=pl.ANY)
    vmem = pl.BlockSpec(memory_space=pltpu.VMEM)
    excess, weights = pl.pallas_call(
        functools.partial(kernel, sizes),
        out_shape=(
            jax.ShapeDtypeStruct((1, tok), jnp.float32),
            jax.ShapeDtypeStruct((1, prior.shape[0]), jnp.float32),
        ),
        in_specs=[anywhere] * 4 + [vmem] * 4,
        out_specs=(vmem, vmem),
        scratch_shapes=[
            pltpu.VMEM((2, ncol, nz, 2 * tok, feats), jnp.bfloat16),
            pltpu.VMEM((2, nz, voc, feats), jnp.bfloat16),
            pltpu.VMEM((2, ncol, voc, 2 * tok), jnp.float32),
            pltpu.VMEM((1, 384), jnp.int32),
            pltpu.VMEM((ndp, 1, 384), jnp.int32),
            pltpu.VMEM((ndev, ncol, 1, 384), jnp.float32),
            pltpu.SemaphoreType.DMA((2,)),
            pltpu.SemaphoreType.DMA((2, nz)),
            pltpu.SemaphoreType.DMA,
            pltpu.SemaphoreType.DMA((2, ncol, nz, 2)),
            pltpu.SemaphoreType.DMA,
            pltpu.SemaphoreType.DMA,
            pltpu.SemaphoreType.DMA,
            pltpu.SemaphoreType.DMA,
        ],
        compiler_params=pltpu.CompilerParams(
            collective_id=0, has_side_effects=True, vmem_limit_bytes=66_000_000
        ),
    )(h0, h1, w0, w1, targets[None], domains[None], keep[None], prior[None])
    return excess[0], weights[0]


def hops(route, dz, da, db, end):
    kind, first = route
    up, down = dz <= 0, dz >= 0 and not end
    along = [step for step, ok in (("u", up), ("d", down)) if ok]
    cross = {"a": da == 0, "b": db == 0}
    here = da == 0 and db == 0
    second = "b" if first == "a" else "a"
    relay = [second] if cross[second] and not cross[first] else []
    if kind == "Z":
        return along + ["a", "b"] if here else relay
    if kind == "P":
        plane = (["a", "b"] if here else relay) if dz == 0 else []
        return plane + along
    if dz == 0 and here:
        return [first] + along + [second]
    return along + [second] if cross[second] else []


def plane_kernel(
    tok,
    hidden0, hidden1, head0, head1, targets, domains, keep, prior,
    excess_out, weights_out,
    gath, heads, acc, own_meta, meta_src, meta, first_weights, member, line, comb, last,
    load_sem, head_sem, small_sem, item_send, item_recv, meta_send, meta_recv,
    line_send, line_recv, comb_send, comb_recv, last_send, last_recv,
):
    nz, ncol = 4, 4
    ndp = 2 * ncol
    voc = head0.shape[0]
    feats = hidden0.shape[1]
    part = feats // 2
    pair = 2 * tok
    dom = prior.shape[1]
    dp = lax.axis_index("dp")
    z = lax.axis_index("tensor")
    core = dp % 2
    col = dp // 2
    a, b = col // 2, col % 2
    me = dp * nz + z
    slot = z * 2 + core
    end = (z == 0) | (z == nz - 1)
    inner = jnp.logical_not(end)
    sign = jnp.where(2 * z < nz - 1, 1, -1)

    def own_rows(c):
        return pl.ds(pl.multiple_of(c * tok, tok), tok)

    loads = []
    for p in range(4):
        m, h = divmod(p, 2)
        loads.append(
            pltpu.make_async_copy(
                (hidden0, hidden1)[m].at[:, h * part : (h + 1) * part],
                gath.at[m, col, z, h, own_rows(core)],
                load_sem.at[p],
            )
        )
        loads[-1].start()
    small = [
        pltpu.make_async_copy(ref, dst, small_sem.at[k])
        for k, (ref, dst) in enumerate(
            ((targets, own_meta.at[0]), (domains, own_meta.at[1]), (keep, own_meta.at[2]), (prior, first_weights))
        )
    ]
    for copy in small:
        copy.start()

    def place(aa, bb, cc, zz):
        return ((aa * 2 + bb) * 2 + cc, zz)

    partner = place(a, b, 1 - core, z)
    across = {
        "a": place(1 - a, b, core, z),
        "b": place(a, 1 - b, core, z),
        "u": place(a, b, core, z + sign),
        "d": place(a, b, core, z - sign),
    }
    barrier = pltpu.get_barrier_semaphore()
    for target in (across["a"], across["b"], across["u"], partner):
        pl.semaphore_signal(barrier, inc=1, device_id=target, device_id_type=MESH)

    @pl.when(inner)
    def _():
        pl.semaphore_signal(barrier, inc=1, device_id=across["d"], device_id_type=MESH)

    head_loads = []
    for m, ref in enumerate((head0, head1)):
        for k in range(nz):
            head_loads.append(
                pltpu.make_async_copy(ref.at[:, k * feats : (k + 1) * feats], heads.at[m, k], head_sem.at[m, k])
            )
    for copy in loads:
        copy.wait()
    for copy in head_loads:
        copy.start()
    pl.semaphore_wait(barrier, jnp.where(end, 4, 5))

    def item_copy(p, colp, zp, c, target):
        m, h = divmod(p, 2)
        block = gath.at[m, colp, zp, h, own_rows(c)]
        return pltpu.make_async_remote_copy(
            src_ref=block, dst_ref=block, send_sem=item_send, recv_sem=item_recv.at[p, colp, zp, c],
            device_id=target, device_id_type=MESH,
        )

    def column(da, db):
        return (1 - a if da else a) * 2 + (1 - b if db else b)

    def locate(entry):
        p, da, db, dz_end, dz_inner = entry
        dz = dz_end if dz_end == dz_inner else jnp.where(end, dz_end, dz_inner)
        return p, column(da, db), z + sign * dz

    sends = [0, 0]

    def take(entry):
        p, colp, zp = locate(entry)
        _, da, db, dz_end, dz_inner = entry
        if da or db or dz_end:
            item_copy(p, colp, zp, core, partner).wait_recv()
        at_end = hops(ROUTES[p], dz_end, da, db, True)
        at_inner = hops(ROUTES[p], dz_inner, da, db, False)
        sends[0] += len(at_end) + 1
        sends[1] += len(at_inner) + 1
        for step in dict.fromkeys(at_inner + at_end):
            copy = item_copy(p, colp, zp, core, across[step])
            if step in at_end and step in at_inner:
                copy.start()
            else:
                pl.when(end if step in at_end else inner)(copy.start)
        item_copy(p, colp, zp, core, partner).start()

    def multiply(p, rel, colp, zp, fresh):
        m, h = divmod(p, 2)
        product = lax.dot_general(
            heads[m, zp, :, h * part : (h + 1) * part], gath[m, colp, zp, h], (((1,), (1,)), ((), ())),
            preferred_element_type=jnp.float32,
        )
        if fresh:
            acc[m, rel] = product
        else:
            acc[m, rel] += product

    everyone = [(da, db, dc) for da in (1, 0) for db in (1, 0) for dc in (1, 0)]

    def other(da, db, dc, zz):
        return place(1 - a if da else a, 1 - b if db else b, 1 - core if dc else core, zz)

    def meta_copy(da, db, dc):
        return pltpu.make_async_remote_copy(
            src_ref=meta_src, dst_ref=meta.at[dp], send_sem=meta_send, recv_sem=meta_recv,
            device_id=other(da, db, dc, z), device_id_type=MESH,
        )

    def meta_row(colp, r):
        low = meta[2 * colp, :, r * 128 : (r + 1) * 128]
        high = meta[2 * colp + 1, :, r * 128 : (r + 1) * 128]
        return low + pltpu.roll(high, tok, 1)

    entries = lax.broadcasted_iota(jnp.int32, (voc, pair), 0) + me * voc
    lane = lax.broadcasted_iota(jnp.int32, (1, 128), 1)
    labels = lax.broadcasted_iota(jnp.int32, (dom, 128), 0)
    steps = lax.broadcasted_iota(jnp.int32, (STEPS, 128), 0)
    row4 = lax.broadcasted_iota(jnp.int32, (4, 128), 0)
    batch = ncol * pair // STEPS
    valid = lane < pair

    order = []
    left = {}
    for p, da, db, _, _ in PLAN:
        left[da, db] = left.get((da, db), 0) + 1
    remaining = dict(left)
    for _, da, db, _, _ in PLAN:
        remaining[da, db] -= 1
        if not remaining[da, db]:
            order.append((da, db))

    def finish(rel, colp, block):
        matched = entries == meta_row(colp, 0)[:, :pair]
        lse, hit = [], []
        for m in (0, 1):
            logits = acc[m, rel]
            peak = jnp.max(logits, axis=0, keepdims=True)
            lse.append(peak + jnp.log(jnp.sum(jnp.exp(logits - peak), axis=0, keepdims=True)))
            hit.append(jnp.sum(jnp.where(matched, logits, 0.0), axis=0, keepdims=True))
        rows = (lse[0], lse[1], hit[0] - hit[1], jnp.zeros_like(hit[0]))
        for r, row in enumerate(rows):
            block[r : r + 1, :pair] = row

    def merge(stack):
        peak = jnp.max(stack, axis=0)
        lse = peak + jnp.log(jnp.sum(jnp.exp(stack - peak[None]), axis=0))
        return jnp.where(row4 < 2, lse, jnp.sum(stack, axis=0))

    def line_copy(r, dc, k):
        return pltpu.make_async_remote_copy(
            src_ref=line.at[r, slot], dst_ref=line.at[r, slot], send_sem=line_send, recv_sem=line_recv,
            device_id=place(a, b, 1 - core if dc else core, lax.rem(z + k, nz)), device_id_type=MESH,
        )

    def comb_copy(da, db):
        return pltpu.make_async_remote_copy(
            src_ref=comb.at[0], dst_ref=comb.at[da * 2 + db], send_sem=comb_send, recv_sem=comb_recv,
            device_id=other(da, db, 0, z), device_id_type=MESH,
        )

    def last_copy(da, db, dc, k):
        return pltpu.make_async_remote_copy(
            src_ref=last.at[slot], dst_ref=last.at[(da * 2 + db) * 2 * nz + slot], send_sem=last_send, recv_sem=last_recv,
            device_id=other(da, db, dc, lax.rem(z + k, nz)), device_id_type=MESH,
        )

    prepared = [None]

    def prepare():
        remote = meta.at[pl.ds(0, ndp - 1)]
        pltpu.make_async_copy(remote, remote, meta_recv).wait()
        counts = jnp.zeros((STEPS, dom), jnp.float32)
        for rel in range(ncol):
            colp = column(*divmod(rel, 2))
            mine = jnp.where((meta_row(colp, 1) == labels) & valid, 1.0, 0.0).astype(jnp.bfloat16)
            member[:, rel * 128 : (rel + 1) * 128] = mine
            step_of = (lane + colp * pair) // batch
            kept = jnp.where((steps == step_of) & valid, meta_row(colp, 2).astype(jnp.float32), 0.0)
            counts = counts + lax.dot_general(
                kept.astype(jnp.bfloat16), mine, (((1,), (1,)), ((), ())), preferred_element_type=jnp.float32
            )
        start = first_weights[...]
        first_weights[...] = start / jnp.sum(start, axis=1, keepdims=True)
        prepared[0] = jnp.maximum(counts, 1.0)

    waiting = []
    heard = set()
    started_meta = [False]
    fresh = set()
    todo = dict(left)
    heads_in = [False]

    def work(entry):
        p, colp, zp = locate(entry)
        _, da, db, dz_end, _ = entry
        item_copy(p, colp, zp, 1 - core, partner).wait_recv()
        if not heads_in[0]:
            heads_in[0] = True
            for copy in head_loads:
                copy.wait()
        rel = da * 2 + db
        key = (p // 2, rel)
        multiply(p, rel, colp, zp, key not in fresh)
        fresh.add(key)
        if dz_end == 0:
            heard.add((da, db))
        if len(heard) == ncol and not started_meta[0]:
            started_meta[0] = True
            for who in everyone[:-1]:
                meta_copy(*who).start()
        todo[da, db] -= 1
        if todo[da, db]:
            return
        if prepared[0] is None:
            prepare()
        r = order.index((da, db))
        if r < ncol - 1:
            finish(rel, colp, line.at[r, slot])
            for k in (3, 2, 1, 0):
                for dc in (1, 0):
                    if k or dc:
                        line_copy(r, dc, k).start()
        else:
            finish(rel, colp, last.at[slot])
            for k in (3, 2, 1, 0):
                for who in everyone:
                    if k or any(who):
                        last_copy(*who, k).start()

    for number, entry in enumerate(PLAN):
        take(entry)
        if number == 3:
            for copy in small:
                copy.wait()
            meta_src[...] = jnp.zeros_like(meta_src)
            for r in range(3):
                meta_src[:, r * 128 : r * 128 + tok] = own_meta[r]
            meta[dp] = meta_src[...]
        waiting.append(entry)
        while len(waiting) > PLAN_LAG or (waiting and number == len(PLAN) - 1):
            work(waiting.pop(0))

    lines = line.at[:, pl.ds(0, 7)]
    pltpu.make_async_copy(lines, lines, line_recv).wait()
    for r in range(ncol - 1):
        comb[0, r] = merge(line[r])
    for da, db in ((1, 1), (0, 1), (1, 0)):
        comb_copy(da, db).start()

    def drain(count):
        for size, block in ((128, gath), (64, gath.at[0]), (16, gath.at[0, 0]), (4, gath.at[0, 0, 0]), (2, gath.at[0, 0, 0, 0]), (1, gath.at[0, 0, 0, 0, pl.ds(0, tok)])):
            while count >= size:
                count -= size
                pltpu.make_async_copy(block, block, item_send).wait()

    pl.when(end)(functools.partial(drain, sends[0]))
    pl.when(inner)(functools.partial(drain, sends[1]))
    sent_meta = meta.at[pl.ds(0, ndp - 1)]
    pltpu.make_async_copy(sent_meta, sent_meta, meta_send).wait()
    pltpu.make_async_copy(lines, lines, line_send).wait()

    combs = comb.at[pl.ds(0, ncol - 1)]
    pltpu.make_async_copy(combs, combs, comb_recv).wait()
    far = last.at[pl.ds(0, ndp * nz - 1)]
    pltpu.make_async_copy(far, far, last_recv).wait()

    rows = []
    own_excess = None
    for rel in range(ncol):
        ra, rb = divmod(rel, 2)
        stack = []
        for part_line in range(ncol):
            la, lb = divmod(part_line, 2)
            r = order.index(((la + ra) % 2, (lb + rb) % 2))
            if r < ncol - 1:
                stack.append(comb[part_line, r][None])
            else:
                stack.append(last[part_line * 2 * nz : (part_line + 1) * 2 * nz])
        merged = merge(jnp.concatenate(stack, axis=0))
        gap = jnp.where(valid, merged[0:1] - merged[1:2] - merged[2:3], 0.0)
        colp = column(ra, rb)
        kept = meta_row(colp, 2).astype(jnp.float32)
        if rel == 0:
            own_excess = gap * kept
        clipped = jnp.maximum(gap, 0.0) * kept
        step_of = (lane + colp * pair) // batch
        rows.append(jnp.where(steps == step_of, clipped, 0.0))
    values = jnp.concatenate(rows, axis=1)
    high = values.astype(jnp.bfloat16)
    rest = values - high.astype(jnp.float32)
    middle = rest.astype(jnp.bfloat16)
    low = (rest - middle.astype(jnp.float32)).astype(jnp.bfloat16)
    sums = jnp.zeros((STEPS, dom), jnp.float32)
    for piece in (low, middle, high):
        sums = sums + lax.dot_general(
            piece, member[...], (((1,), (1,)), ((), ())), preferred_element_type=jnp.float32
        )
    mine = jnp.where(core == 0, own_excess, pltpu.roll(own_excess, 128 - tok, 1))
    excess_out[...] = mine[:, :tok]
    growth = jnp.exp(step_size * (sums / prepared[0]))
    weights = first_weights[...]
    for s in range(STEPS):
        raised = weights * growth[s : s + 1]
        weights = (1.0 - smoothing) * raised / jnp.sum(raised, axis=1, keepdims=True) + smoothing / dom
    weights_out[...] = jnp.log(weights)

    pltpu.make_async_copy(combs, combs, comb_send).wait()
    pltpu.make_async_copy(far, far, last_send).wait()


def plane_local(h0, h1, w0, w1, targets, domains, keep, prior):
    tok, feats = h0.shape
    voc = w0.shape[0]
    dom = prior.shape[0]
    hbm = pl.BlockSpec(memory_space=pltpu.HBM)
    vmem = pl.BlockSpec(memory_space=pltpu.VMEM)
    excess, weights = pl.pallas_call(
        functools.partial(plane_kernel, tok),
        out_shape=(
            jax.ShapeDtypeStruct((1, tok), jnp.float32),
            jax.ShapeDtypeStruct((1, dom), jnp.float32),
        ),
        in_specs=[hbm] * 8,
        out_specs=(vmem, vmem),
        scratch_shapes=[
            pltpu.VMEM((2, 4, 4, 2, 2 * tok, feats // 2), jnp.bfloat16),
            pltpu.VMEM((2, 4, voc, feats), jnp.bfloat16),
            pltpu.VMEM((2, 4, voc, 2 * tok), jnp.float32),
            pltpu.VMEM((3, 1, tok), jnp.int32),
            pltpu.VMEM((1, 384), jnp.int32),
            pltpu.VMEM((8, 1, 384), jnp.int32),
            pltpu.VMEM((1, dom), jnp.float32),
            pltpu.VMEM((dom, 512), jnp.bfloat16),
            pltpu.VMEM((3, 8, 4, 128), jnp.float32),
            pltpu.VMEM((4, 3, 4, 128), jnp.float32),
            pltpu.VMEM((32, 4, 128), jnp.float32),
            pltpu.SemaphoreType.DMA((4,)),
            pltpu.SemaphoreType.DMA((2, 4)),
            pltpu.SemaphoreType.DMA((4,)),
            pltpu.SemaphoreType.DMA,
            pltpu.SemaphoreType.DMA((4, 4, 4, 2)),
        ]
        + [pltpu.SemaphoreType.DMA] * 8,
        compiler_params=pltpu.CompilerParams(
            collective_id=0, has_side_effects=True, vmem_limit_bytes=66_000_000
        ),
    )(h0, h1, w0, w1, targets[None], domains[None], keep[None], prior[None])
    return excess[0], weights[0]


def solution(mesh):
    ndp, nz = mesh.shape["dp"], mesh.shape["tensor"]
    ncol = ndp // 2
    rows_b = max(k for k in range(1, ncol + 1) if ncol % k == 0 and k * k <= ncol)

    def body(h0, *rest):
        if (ncol // rows_b, rows_b, nz) == (2, 2, 4):
            return plane_local(h0, *rest)
        return local((ncol // rows_b, rows_b, nz, h0.shape[0]), h0, *rest)

    in_specs = (
        P("dp", "tensor"),
        P("dp", "tensor"),
        P(("dp", "tensor"), None),
        P(("dp", "tensor"), None),
        P("dp"),
        P("dp"),
        P("dp"),
        P(),
    )
    return jax.shard_map(body, mesh=mesh, in_specs=in_specs, out_specs=(P("dp"), P()), check_vma=False)
```
